32 devices in a mesh: groups: 2 (over x), ctx: 16 (over z, y, core), tp: 1.
Axes of the slice: x: 2, y: 2, z: 4, core: 2. Of those that a mesh axis runs over, the one named last changes fastest.
Arguments:
- query_states: bfloat16 [8192, 32, 128], P(('groups', 'ctx'), 'tp'), parts along dimension 0, may hold values from -8 to 8
- key_states: bfloat16 [8192, 4, 128], P(('groups', 'ctx'), 'tp'), parts along dimension 0, may hold values from -8 to 8
- value_rows: bfloat16 [8192, 4, 128], P(('groups', 'ctx'), 'tp'), parts along dimension 0, may hold values from -12 to 12
- positions: int32 [8192], P(('groups', 'ctx')), parts along dimension 0, may hold values from 0 to 4095, as said below
- out_weight: bfloat16 [4096, 4096], P('tp', 'ctx'), may hold values from -0.375 to 0.375
Outputs:
- projected: bfloat16 [8192, 4096], P(('groups', 'ctx'), 'tp'), parts along dimension 0
The draws below stay inside these ranges and needn't reach their ends.
There are 2 independent parts, one for each index of `groups`. The reference program is written for one: setup_inputs(seed, part) draws one part's arguments, and reference() takes and returns one part's arrays. A program takes and returns all parts, laid end to end along the dimension named above; an argument that names none is the same for every part. Nothing has to cross between parts.
Inputs may be any that keep to these rules, and one draw needn't show every extreme that they name: Each of 0 to 4095 appears once. Half-block b holds positions b * 128 to (b + 1) * 128 - 1. The 256 rows of one device along ctx hold half-block j and then half-block 32 - 1 - j, each in rising order, for a j below 16 that differs from device to device.
All inputs are finite; a program needn't handle non-finite values.
Results may differ from the reference program's by a relative error of at most 0.01.
Values may be sent and summed in bfloat16 or wider, within the bound.
A program may use at most 128 MiB of HBM per device.

```python
from functools import partial
import jax
import jax.numpy as jnp
from jax import lax

QUERY_HEAD_COUNT = 32
KEY_VALUE_HEADS = 4
HEAD_WIDTH = 128
DOUT = 4096
HALF = 128
SEQUENCE_LENGTH = 4096
HALF_BLOCK_COUNT = 32


def draw_query_states(key, part):
    base_point = jax.random.fold_in(key, 21)
    value_entries = jnp.clip(jax.random.normal(jax.random.fold_in(base_point, 1), (SEQUENCE_LENGTH, QUERY_HEAD_COUNT, HEAD_WIDTH)), -8.0, 8.0)
    return value_entries.astype(jnp.bfloat16)


def draw_key_states(key, part):
    base_point = jax.random.fold_in(key, 41)
    value_entries = jnp.clip(jax.random.normal(jax.random.fold_in(base_point, 1), (SEQUENCE_LENGTH, KEY_VALUE_HEADS, HEAD_WIDTH)), -8.0, 8.0)
    return value_entries.astype(jnp.bfloat16)


def draw_positions(key, part):
    order = jax.random.permutation(jax.random.fold_in(key, 31), HALF_BLOCK_COUNT // 2)
    within = jnp.arange(HALF)
    lower = order[:, None] * HALF + within[None, :]
    upper = (HALF_BLOCK_COUNT - 1 - order)[:, None] * HALF + within[None, :]
    return jnp.concatenate([lower, upper], axis=1).reshape(SEQUENCE_LENGTH).astype(jnp.int32)


def steps_of(stream_key, dims, cuts, low, top_value):
    loudness = 1.0
    for dim, parts in cuts:
        steps = jax.random.uniform(jax.random.fold_in(jax.random.fold_in(stream_key, 6), dim), (parts,), jnp.float32, low / len(cuts), top_value / len(cuts))
        loudness = loudness * jnp.repeat(jnp.exp(steps), dims[dim] // parts).reshape((-1,) + (1,) * (len(dims) - 1 - dim))
    return loudness


def gaussian(key, shape, scale, limit, shards=(), dtype=jnp.bfloat16):
    loudness = steps_of(key, shape, shards, -0.22, 0.18) if shards else 1.0
    values = jax.random.normal(key, shape, jnp.float32) * scale * loudness
    return jnp.minimum(jnp.maximum(values, -limit), limit).astype(dtype)


def setup_inputs(seed: int = 0, part: int = 0) -> dict:
    streams_of = jax.random.split(jax.random.key(seed), 6)
    part_splits = jax.random.split(jax.random.fold_in(streams_of[5], part), 6)
    query_states = draw_query_states(jax.random.fold_in(jax.random.fold_in(streams_of[5], part), 71), part)
    key_states = draw_key_states(jax.random.fold_in(jax.random.fold_in(streams_of[5], part), 71), part)
    value_rows = gaussian(part_splits[2], (SEQUENCE_LENGTH, KEY_VALUE_HEADS, HEAD_WIDTH), 2.0, 12.0, ((0, 16),))
    positions = draw_positions(jax.random.fold_in(jax.random.fold_in(streams_of[5], part), 71), part)
    out_weight = gaussian(streams_of[4], (QUERY_HEAD_COUNT * HEAD_WIDTH, DOUT), (QUERY_HEAD_COUNT * HEAD_WIDTH // 16) ** -0.5, 0.375, ((1, 16),))
    return {"query_states": query_states, "key_states": key_states, "value_rows": value_rows, "positions": positions, "out_weight": out_weight}


def one_head(operands, visible):
    query_head, key_head, value_head = operands
    scores = jnp.dot(query_head, key_head.T, preferred_element_type=jnp.float32) * (HEAD_WIDTH ** -0.5)
    scores = jnp.where(visible, scores, -jnp.inf)
    largest = jnp.max(scores, axis=1)
    exp_scores = jnp.exp(scores - largest[:, None])
    denominator = jnp.sum(exp_scores, axis=1)
    weighted = jnp.dot(exp_scores.astype(jnp.bfloat16), value_head, preferred_element_type=jnp.float32)
    return (weighted / denominator[:, None]).astype(jnp.bfloat16)


def reference(query_states, key_states, value_rows, positions, out_weight):
    visible = positions[None, :] <= positions[:, None]
    group_width = QUERY_HEAD_COUNT // KEY_VALUE_HEADS
    query_major = jnp.moveaxis(query_states, 1, 0)
    key_major = jnp.repeat(jnp.moveaxis(key_states, 1, 0), group_width, axis=0)
    value_major = jnp.repeat(jnp.moveaxis(value_rows, 1, 0), group_width, axis=0)
    attended = lax.map(partial(one_head, visible=visible), (query_major, key_major, value_major))
    attended = jnp.moveaxis(attended, 0, 1).reshape(SEQUENCE_LENGTH, QUERY_HEAD_COUNT * HEAD_WIDTH)
    return jnp.dot(attended, out_weight, preferred_element_type=jnp.float32).astype(jnp.bfloat16)
```

```python
import functools
import math

import jax
import jax.numpy as jnp
from jax import lax
from jax.experimental import pallas as pl
from jax.experimental.pallas import tpu as pltpu
from jax.sharding import PartitionSpec as P

LOW_START = -1e30
BLOCKS_PER_STEP = 4
CHUNK = 256


def attend_kernel(half, group, place_ref, own_ref, q_ref, k_ref, v_ref, out_ref, acc_ref, max_ref, sum_ref):
    rows = group * half
    head_size = q_ref.shape[-1]
    span = BLOCKS_PER_STEP * half
    chunk = min(CHUNK, rows)
    to_exp2 = head_size ** (-0.5) * math.log2(math.e)

    def step(which, number, masked, query_block):
        keys, values = [], []
        for i in range(BLOCKS_PER_STEP):
            place = place_ref[number * BLOCKS_PER_STEP + i]
            keys.append(k_ref[pl.ds(pl.multiple_of(place * half, half), half), :])
            values.append(v_ref[pl.ds(pl.multiple_of(place * half, half), half), :])
        key_part = jnp.concatenate(keys, axis=0)
        value_part = jnp.concatenate(values, axis=0)
        if masked:
            key_place = number * span + lax.broadcasted_iota(jnp.int32, (span, chunk), 0)
            query_place = query_block * half + lax.broadcasted_iota(jnp.int32, (span, chunk), 1) % half
            visible = key_place <= query_place
        for c in range(rows // chunk):
            cols = pl.ds(c * chunk, chunk)
            scores = lax.dot_general(
                key_part,
                q_ref[0, which, cols, :],
                (((1,), (1,)), ((), ())),
                preferred_element_type=jnp.float32,
            )
            if masked:
                scores = jnp.where(visible, scores, LOW_START)
            old_max = max_ref[:, cols]
            new_max = jnp.maximum(old_max, jnp.max(scores, axis=0, keepdims=True))
            factor = jnp.exp2((old_max - new_max) * to_exp2)
            exp_scores = jnp.exp2((scores - new_max) * to_exp2)
            max_ref[:, cols] = new_max
            sum_ref[:, cols] = sum_ref[:, cols] * factor + jnp.sum(exp_scores, axis=0, keepdims=True)
            weighted = lax.dot_general(
                value_part,
                exp_scores.astype(jnp.bfloat16),
                (((0,), (0,)), ((), ())),
                preferred_element_type=jnp.float32,
            )
            acc_ref[:, cols] = acc_ref[:, cols] * factor + weighted

    for which in range(2):
        query_block = own_ref[which]
        steps = query_block // BLOCKS_PER_STEP
        max_ref[...] = jnp.full_like(max_ref, LOW_START)
        sum_ref[...] = jnp.zeros_like(sum_ref)
        acc_ref[...] = jnp.zeros_like(acc_ref)

        @pl.loop(0, steps)
        def _(number):
            step(which, number, False, query_block)

        step(which, steps, True, query_block)
        for g in range(group):
            cols = pl.ds(g * half, half)
            attended = acc_ref[:, cols] / sum_ref[:, cols]
            out_ref[pl.ds(g * head_size, head_size), pl.ds(which * half, half)] = attended.astype(jnp.bfloat16)


def attend(query_parts, gathered, place, own, first_head, all_heads):
    kv_heads, _, rows, head_size = query_parts.shape
    keys_total = gathered.shape[0]
    blocks = place.shape[0]
    half = keys_total // blocks
    group = rows // half
    flops = 4 * kv_heads * rows * head_size * half * (blocks + 1)
    return pl.pallas_call(
        functools.partial(attend_kernel, half, group),
        out_shape=jax.ShapeDtypeStruct((kv_heads * group * head_size, 2 * half), jnp.bfloat16),
        grid_spec=pltpu.PrefetchScalarGridSpec(
            num_scalar_prefetch=2,
            grid=(kv_heads,),
            in_specs=[
                pl.BlockSpec((1, 2, rows, head_size), lambda h, *_: (h, 0, 0, 0)),
                pl.BlockSpec((keys_total, head_size), lambda h, *_: (0, h + first_head)),
                pl.BlockSpec((keys_total, head_size), lambda h, *_: (0, h + first_head + all_heads)),
            ],
            out_specs=pl.BlockSpec((group * head_size, 2 * half), lambda h, *_: (h, 0)),
            scratch_shapes=[
                pltpu.VMEM((head_size, rows), jnp.float32),
                pltpu.VMEM((1, rows), jnp.float32),
                pltpu.VMEM((1, rows), jnp.float32),
            ],
        ),
        compiler_params=pltpu.CompilerParams(
            dimension_semantics=("arbitrary",), vmem_limit_bytes=40 * 1024 * 1024
        ),
        cost_estimate=pl.CostEstimate(
            flops=flops, bytes_accessed=2 * gathered.size, transcendentals=flops // (4 * head_size)
        ),
        name="attend",
    )(place, own, query_parts, gathered, gathered)


def spread_kernel(devices, own_ref, out_ref, far_send, far_recv, side_send, side_recv, pair_send, pair_recv, own_sem):
    me = lax.axis_index("ctx")
    outers = devices // 4
    outer, middle, inner = me // 4, (me // 2) % 2, me % 2

    def at(o, m, i):
        return (o * 2 + m) * 2 + i

    side = at(outer, 1 - middle, inner)
    pair = at(outer, middle, 1 - inner)
    far = [at((outer + k) % outers, middle, inner) for k in range(1, outers)]
    barrier = pltpu.get_barrier_semaphore()
    for other in far + [side, pair]:
        pl.semaphore_signal(barrier, inc=1, device_id={"ctx": other}, device_id_type=pl.DeviceIdType.MESH)
    pl.semaphore_wait(barrier, outers + 1)

    def send(source, slot, sends, recvs, number, target):
        return pltpu.make_async_remote_copy(
            src_ref=source,
            dst_ref=out_ref.at[slot],
            send_sem=sends.at[number],
            recv_sem=recvs.at[number],
            device_id={"ctx": target},
            device_id_type=pl.DeviceIdType.MESH,
        )

    own = pltpu.make_async_copy(own_ref, out_ref.at[me], own_sem)
    far_copies = [send(own_ref, me, far_send, far_recv, k, far[k]) for k in range(outers - 1)]
    for copy in far_copies:
        copy.start()
    side_copies = [send(own_ref, me, side_send, side_recv, 0, side)]
    pair_copies = [send(own_ref, me, pair_send, pair_recv, 0, pair)]
    side_copies[0].start()
    pair_copies[0].start()
    own.start()
    for k in range(outers - 1):
        far_copies[k].wait_recv()
        slot = at((outer + outers - 1 - k) % outers, middle, inner)
        side_copies.append(send(out_ref.at[slot], slot, side_send, side_recv, k + 1, side))
        pair_copies.append(send(out_ref.at[slot], slot, pair_send, pair_recv, k + 1, pair))
        side_copies[-1].start()
        pair_copies[-1].start()
    for k in range(outers):
        side_copies[k].wait_recv()
        slot = at((outer + outers - k) % outers, 1 - middle, inner)
        pair_copies.append(send(out_ref.at[slot], slot, pair_send, pair_recv, outers + k, pair))
        pair_copies[-1].start()
    for copy in pair_copies:
        copy.wait_recv()
    for copy in far_copies + side_copies + pair_copies:
        copy.wait_send()
    own.wait()


def spread(packed):
    devices = lax.axis_size("ctx")
    outers = devices // 4
    rows, columns = packed.shape
    gathered = pl.pallas_call(
        functools.partial(spread_kernel, devices),
        out_shape=jax.ShapeDtypeStruct((devices, rows, columns), packed.dtype),
        in_specs=[pl.BlockSpec(memory_space=pltpu.VMEM)],
        out_specs=pl.BlockSpec(memory_space=pltpu.VMEM),
        scratch_shapes=[
            pltpu.SemaphoreType.DMA((outers - 1,)),
            pltpu.SemaphoreType.DMA((outers - 1,)),
            pltpu.SemaphoreType.DMA((outers,)),
            pltpu.SemaphoreType.DMA((outers,)),
            pltpu.SemaphoreType.DMA((2 * outers,)),
            pltpu.SemaphoreType.DMA((2 * outers,)),
            pltpu.SemaphoreType.DMA,
        ],
        compiler_params=pltpu.CompilerParams(
            collective_id=0, has_side_effects=True, vmem_limit_bytes=24 * 1024 * 1024
        ),
        cost_estimate=pl.CostEstimate(flops=0, bytes_accessed=20 * packed.size * devices, transcendentals=0),
        name="spread",
    )(packed)
    return gathered.reshape(devices * rows, columns)


def hand_on(value, by):
    parts = lax.axis_size("groups")
    return lax.ppermute(value, "groups", [(i, (i + by) % parts) for i in range(parts)])


def local(query_states, key_states, value_rows, positions, out_weight):
    tokens, query_heads, head_size = query_states.shape
    kv_heads = key_states.shape[1]
    group = query_heads // kv_heads
    half = tokens // 2
    devices = lax.axis_size("ctx")
    blocks = 2 * devices
    parts = lax.axis_size("groups")
    me_part = lax.axis_index("groups")
    share = out_weight.shape[1] // parts
    weight_share = lax.dynamic_slice_in_dim(out_weight, me_part * share, share, 1)
    weight = lax.all_gather(weight_share, "ctx", axis=1, tiled=True)
    packed = jnp.concatenate(
        [key_states.reshape(tokens, kv_heads * head_size), value_rows.reshape(tokens, kv_heads * head_size)], axis=1
    )
    first = positions[0] // half
    firsts = lax.all_gather(first, "ctx")
    gathered = spread(packed)
    wanted = jnp.arange(blocks, dtype=jnp.int32)[:, None]
    stored = jnp.stack([firsts, blocks - 1 - firsts], axis=1).reshape(1, blocks)
    place = jnp.sum(jnp.where(stored == wanted, jnp.arange(blocks, dtype=jnp.int32)[None, :], 0), axis=1)
    place = place.astype(jnp.int32)
    own = jnp.stack([first, blocks - 1 - first]).astype(jnp.int32)
    query_parts = query_states.reshape(2, half, kv_heads, group, head_size).transpose(2, 0, 3, 1, 4)
    query_parts = query_parts.reshape(kv_heads, 2, group * half, head_size)
    pieces = min(2, kv_heads)
    span = kv_heads // pieces
    attended = [
        attend(query_parts[i * span : (i + 1) * span], gathered, place, own, i * span, kv_heads) for i in range(pieces)
    ]

    def project(rows):
        product = lax.dot_general(
            jnp.concatenate(rows, axis=0), weight, (((0,), (0,)), ((), ())), preferred_element_type=jnp.float32
        )
        return product.astype(jnp.bfloat16)

    guests = [[hand_on(piece, by) for piece in attended] for by in range(1, parts)]
    mine = project(attended)
    results = [mine] + [hand_on(project(rows), parts - 1 - i) for i, rows in enumerate(guests)]
    shares = jnp.stack([r.reshape(tokens, devices, share) for r in results])
    order = (jnp.arange(parts) - me_part) % parts
    if parts == 2:
        low = jnp.where(me_part == 0, shares[0], shares[1])
        high = jnp.where(me_part == 0, shares[1], shares[0])
        combined = jnp.stack([low, high], axis=2)
    else:
        combined = jnp.moveaxis(jnp.take(shares, order, axis=0), 0, 2)
    combined = combined.reshape(tokens, devices * parts * share)
    return lax.psum_scatter(combined, "tp", scatter_dimension=1, tiled=True)


def solution(mesh):
    in_specs = (
        P(("groups", "ctx"), "tp", None),
        P(("groups", "ctx"), "tp", None),
        P(("groups", "ctx"), "tp", None),
        P(("groups", "ctx")),
        P("tp", "ctx"),
    )
    out_specs = P(("groups", "ctx"), "tp")
    return jax.shard_map(local, mesh=mesh, in_specs=in_specs, out_specs=out_specs, check_vma=False)
```

```python
import functools
import math

import jax
import jax.numpy as jnp
from jax import lax
from jax.experimental import pallas as pl
from jax.experimental.pallas import tpu as pltpu
from jax.sharding import PartitionSpec as P

LOW_START = -1e30
BLOCKS_PER_STEP = 4
CHUNK = 1024
TAIL = 16


def attend_kernel(half, group, place_ref, own_ref, q_ref, k_ref, v_ref, out_ref, acc_ref, max_ref, sum_ref):
    rows = group * half
    head_size = q_ref.shape[-1]
    span = BLOCKS_PER_STEP * half
    chunk = min(CHUNK, rows)
    to_exp2 = head_size ** (-0.5) * math.log2(math.e)

    def step(which, number, masked, query_block):
        keys, values = [], []
        for i in range(BLOCKS_PER_STEP):
            place = place_ref[number * BLOCKS_PER_STEP + i]
            keys.append(k_ref[pl.ds(pl.multiple_of(place, TAIL), half), :])
            values.append(v_ref[pl.ds(pl.multiple_of(place, TAIL), half), :])
        key_part = jnp.concatenate(keys, axis=0)
        value_part = jnp.concatenate(values, axis=0)
        if masked:
            key_place = number * span + lax.broadcasted_iota(jnp.int32, (span, chunk), 0)
            query_place = query_block * half + lax.broadcasted_iota(jnp.int32, (span, chunk), 1) % half
            visible = key_place <= query_place
        for c in range(rows // chunk):
            cols = pl.ds(c * chunk, chunk)
            scores = lax.dot_general(
                key_part,
                q_ref[0, which, cols, :],
                (((1,), (1,)), ((), ())),
                preferred_element_type=jnp.float32,
            )
            if masked:
                scores = jnp.where(visible, scores, LOW_START)
            old_max = max_ref[:, cols]
            new_max = jnp.maximum(old_max, jnp.max(scores, axis=0, keepdims=True))
            factor = jnp.exp2((old_max - new_max) * to_exp2)
            exp_scores = jnp.exp2((scores - new_max) * to_exp2)
            max_ref[:, cols] = new_max
            sum_ref[:, cols] = sum_ref[:, cols] * factor + jnp.sum(exp_scores, axis=0, keepdims=True)
            weighted = lax.dot_general(
                value_part,
                exp_scores.astype(jnp.bfloat16),
                (((0,), (0,)), ((), ())),
                preferred_element_type=jnp.float32,
            )
            acc_ref[:, cols] = acc_ref[:, cols] * factor + weighted

    for which in range(2):
        query_block = own_ref[which]
        steps = query_block // BLOCKS_PER_STEP
        max_ref[...] = jnp.full_like(max_ref, LOW_START)
        sum_ref[...] = jnp.zeros_like(sum_ref)
        acc_ref[...] = jnp.zeros_like(acc_ref)

        @pl.loop(0, steps)
        def _(number):
            step(which, number, False, query_block)

        step(which, steps, True, query_block)
        for g in range(group):
            cols = pl.ds(g * half, half)
            attended = acc_ref[:, cols] / sum_ref[:, cols]
            out_ref[pl.ds(g * head_size, head_size), pl.ds(which * half, half)] = attended.astype(jnp.bfloat16)


def attend(query_parts, gathered, place, own, first_head, all_heads, half):
    kv_heads, _, rows, head_size = query_parts.shape
    keys_total = gathered.shape[0]
    blocks = place.shape[0]
    group = rows // half
    flops = 4 * kv_heads * rows * head_size * half * (blocks + 1)
    return pl.pallas_call(
        functools.partial(attend_kernel, half, group),
        out_shape=jax.ShapeDtypeStruct((kv_heads * group * head_size, 2 * half), jnp.bfloat16),
        grid_spec=pltpu.PrefetchScalarGridSpec(
            num_scalar_prefetch=2,
            grid=(kv_heads,),
            in_specs=[
                pl.BlockSpec((1, 2, rows, head_size), lambda h, *_: (h, 0, 0, 0)),
                pl.BlockSpec((keys_total, head_size), lambda h, *_: (0, h + first_head)),
                pl.BlockSpec((keys_total, head_size), lambda h, *_: (0, h + first_head + all_heads)),
            ],
            out_specs=pl.BlockSpec((group * head_size, 2 * half), lambda h, *_: (h, 0)),
            scratch_shapes=[
                pltpu.VMEM((head_size, rows), jnp.float32),
                pltpu.VMEM((1, rows), jnp.float32),
                pltpu.VMEM((1, rows), jnp.float32),
            ],
        ),
        compiler_params=pltpu.CompilerParams(
            dimension_semantics=("arbitrary",), vmem_limit_bytes=20 * 1024 * 1024
        ),
        cost_estimate=pl.CostEstimate(
            flops=flops, bytes_accessed=2 * gathered.size, transcendentals=flops // (4 * head_size)
        ),
        name="attend",
    )(place, own, query_parts, gathered, gathered)


def spread_kernel(devices, own_ref, out_ref, far_send, far_recv, side_send, side_recv, pair_send, pair_recv, own_sem):
    me = lax.axis_index("ctx")
    outers = devices // 4
    outer, middle, inner = me // 4, (me // 2) % 2, me % 2

    def at(o, m, i):
        return (o * 2 + m) * 2 + i

    side = at(outer, 1 - middle, inner)
    pair = at(outer, middle, 1 - inner)
    far = [at((outer + k) % outers, middle, inner) for k in range(1, outers)]
    barrier = pltpu.get_barrier_semaphore()
    for other in far + [side, pair]:
        pl.semaphore_signal(barrier, inc=1, device_id={"ctx": other}, device_id_type=pl.DeviceIdType.MESH)
    pl.semaphore_wait(barrier, outers + 1)

    def send(source, slot, sends, recvs, number, target):
        return pltpu.make_async_remote_copy(
            src_ref=source,
            dst_ref=out_ref.at[slot],
            send_sem=sends.at[number],
            recv_sem=recvs.at[number],
            device_id={"ctx": target},
            device_id_type=pl.DeviceIdType.MESH,
        )

    own = pltpu.make_async_copy(own_ref, out_ref.at[me], own_sem)
    far_copies = [send(own_ref, me, far_send, far_recv, k, far[k]) for k in range(outers - 1)]
    for copy in far_copies:
        copy.start()
    side_copies = [send(own_ref, me, side_send, side_recv, 0, side)]
    pair_copies = [send(own_ref, me, pair_send, pair_recv, 0, pair)]
    side_copies[0].start()
    pair_copies[0].start()
    own.start()
    for k in range(outers - 1):
        far_copies[k].wait_recv()
        slot = at((outer + outers - 1 - k) % outers, middle, inner)
        side_copies.append(send(out_ref.at[slot], slot, side_send, side_recv, k + 1, side))
        pair_copies.append(send(out_ref.at[slot], slot, pair_send, pair_recv, k + 1, pair))
        side_copies[-1].start()
        pair_copies[-1].start()
    for k in range(outers):
        side_copies[k].wait_recv()
        slot = at((outer + outers - k) % outers, 1 - middle, inner)
        pair_copies.append(send(out_ref.at[slot], slot, pair_send, pair_recv, outers + k, pair))
        pair_copies[-1].start()
    for copy in pair_copies:
        copy.wait_recv()
    for copy in far_copies + side_copies + pair_copies:
        copy.wait_send()
    own.wait()


def spread(packed):
    devices = lax.axis_size("ctx")
    outers = devices // 4
    rows, columns = packed.shape
    gathered = pl.pallas_call(
        functools.partial(spread_kernel, devices),
        out_shape=jax.ShapeDtypeStruct((devices, rows, columns), packed.dtype),
        in_specs=[pl.BlockSpec(memory_space=pltpu.VMEM)],
        out_specs=pl.BlockSpec(memory_space=pltpu.VMEM),
        scratch_shapes=[
            pltpu.SemaphoreType.DMA((outers - 1,)),
            pltpu.SemaphoreType.DMA((outers - 1,)),
            pltpu.SemaphoreType.DMA((outers,)),
            pltpu.SemaphoreType.DMA((outers,)),
            pltpu.SemaphoreType.DMA((2 * outers,)),
            pltpu.SemaphoreType.DMA((2 * outers,)),
            pltpu.SemaphoreType.DMA,
        ],
        compiler_params=pltpu.CompilerParams(
            collective_id=0, has_side_effects=True, vmem_limit_bytes=24 * 1024 * 1024
        ),
        cost_estimate=pl.CostEstimate(flops=0, bytes_accessed=20 * packed.size * devices, transcendentals=0),
        name="spread",
    )(packed)
    return gathered


def hand_on(value, by):
    parts = lax.axis_size("groups")
    return lax.ppermute(value, "groups", [(i, (i + by) % parts) for i in range(parts)])


def weave_kernel(me_ref, *refs):
    *shares, out_ref = refs
    parts = len(shares)
    share = shares[0].shape[1]
    for p in range(parts):
        by = lax.rem(p - me_ref[0] + parts, parts)
        chosen = shares[0][...]
        for k in range(1, parts):
            chosen = jnp.where(by == k, shares[k][...], chosen)
        out_ref[:, p * share : (p + 1) * share] = chosen


def weave(results, me_part, devices):
    parts = len(results)
    tokens, columns = results[0].shape
    share = columns // devices
    return pl.pallas_call(
        weave_kernel,
        out_shape=jax.ShapeDtypeStruct((tokens, parts * columns), results[0].dtype),
        grid_spec=pltpu.PrefetchScalarGridSpec(
            num_scalar_prefetch=1,
            grid=(devices,),
            in_specs=[pl.BlockSpec((tokens, share), lambda i, *_: (0, i))] * parts,
            out_specs=pl.BlockSpec((tokens, parts * share), lambda i, *_: (0, i)),
        ),
        name="weave",
    )(me_part.astype(jnp.int32).reshape(1), *results)


def local(query_states, key_states, value_rows, positions, out_weight):
    tokens, query_heads, head_size = query_states.shape
    kv_heads = key_states.shape[1]
    group = query_heads // kv_heads
    half = tokens // 2
    devices = lax.axis_size("ctx")
    blocks = 2 * devices
    parts = lax.axis_size("groups")
    me_part = lax.axis_index("groups")
    share = out_weight.shape[1] // parts
    weight_share = lax.dynamic_slice_in_dim(out_weight, me_part * share, share, 1)
    packed = jnp.concatenate(
        [key_states.reshape(tokens, kv_heads * head_size), value_rows.reshape(tokens, kv_heads * head_size)], axis=1
    )
    first = positions[0] // half
    tail = jnp.broadcast_to(first.astype(packed.dtype), (TAIL, packed.shape[1]))
    gathered = spread(jnp.concatenate([packed, tail], axis=0))
    firsts = gathered[:, tokens, 0].astype(jnp.int32)
    firsts, weight_share = lax.optimization_barrier((firsts, weight_share))
    weight = lax.all_gather(weight_share, "ctx", axis=1, tiled=True)
    gathered = gathered.reshape(devices * (tokens + TAIL), packed.shape[1])
    wanted = jnp.arange(blocks, dtype=jnp.int32)[:, None]
    stored = jnp.stack([firsts, blocks - 1 - firsts], axis=1).reshape(1, blocks)
    kept = jnp.arange(blocks, dtype=jnp.int32)[None, :]
    starts = kept // 2 * (tokens + TAIL) + kept % 2 * half
    place = jnp.sum(jnp.where(stored == wanted, starts, 0), axis=1)
    place = place.astype(jnp.int32)
    own = jnp.stack([first, blocks - 1 - first]).astype(jnp.int32)
    query_parts = query_states.reshape(2, half, kv_heads, group, head_size).transpose(2, 0, 3, 1, 4)
    query_parts = query_parts.reshape(kv_heads, 2, group * half, head_size)
    pieces = min(2, kv_heads)
    span = kv_heads // pieces
    attended = [
        attend(query_parts[i * span : (i + 1) * span], gathered, place, own, i * span, kv_heads, half) for i in range(pieces)
    ]

    def project(rows):
        product = lax.dot_general(
            jnp.concatenate(rows, axis=0), weight, (((0,), (0,)), ((), ())), preferred_element_type=jnp.float32
        )
        return product.astype(jnp.bfloat16)

    guests = [[hand_on(piece, by) for piece in attended] for by in range(1, parts)]
    mine = project(attended)
    results = [mine] + [hand_on(project(rows), parts - 1 - i) for i, rows in enumerate(guests)]
    if share % 128 == 0:
        combined = weave(results, me_part, devices)
    else:
        shares = jnp.stack([r.reshape(tokens, devices, share) for r in results])
        order = (jnp.arange(parts) - me_part) % parts
        combined = jnp.moveaxis(jnp.take(shares, order, axis=0), 0, 2).reshape(tokens, devices * parts * share)
    return lax.psum_scatter(combined, "tp", scatter_dimension=1, tiled=True)


def solution(mesh):
    in_specs = (
        P(("groups", "ctx"), "tp", None),
        P(("groups", "ctx"), "tp", None),
        P(("groups", "ctx"), "tp", None),
        P(("groups", "ctx")),
        P("tp", "ctx"),
    )
    out_specs = P(("groups", "ctx"), "tp")
    return jax.shard_map(local, mesh=mesh, in_specs=in_specs, out_specs=out_specs, check_vma=False)
```

```python
import functools
import math

import jax
import jax.numpy as jnp
from jax import lax
from jax.experimental import pallas as pl
from jax.experimental.pallas import tpu as pltpu
from jax.sharding import PartitionSpec as P

LOW_START = -1e30
BLOCKS_PER_STEP = 4
CHUNK = 1024
TAIL = 16


def attend_kernel(half, group, place_ref, own_ref, q_ref, k_ref, v_ref, out_ref, acc_ref, max_ref, sum_ref):
    rows = group * half
    head_size = q_ref.shape[-1]
    span = BLOCKS_PER_STEP * half
    chunk = min(CHUNK, rows)
    to_exp2 = head_size ** (-0.5) * math.log2(math.e)

    def step(which, number, masked, query_block):
        keys, values = [], []
        for i in range(BLOCKS_PER_STEP):
            place = place_ref[number * BLOCKS_PER_STEP + i]
            keys.append(k_ref[pl.ds(pl.multiple_of(place, TAIL), half), :])
            values.append(v_ref[pl.ds(pl.multiple_of(place, TAIL), half), :])
        key_part = jnp.concatenate(keys, axis=0)
        value_part = jnp.concatenate(values, axis=0)
        if masked:
            key_place = number * span + lax.broadcasted_iota(jnp.int32, (span, chunk), 0)
            query_place = query_block * half + lax.broadcasted_iota(jnp.int32, (span, chunk), 1) % half
            visible = key_place <= query_place
        for c in range(rows // chunk):
            cols = pl.ds(c * chunk, chunk)
            scores = lax.dot_general(
                key_part,
                q_ref[0, which, cols, :],
                (((1,), (1,)), ((), ())),
                preferred_element_type=jnp.float32,
            )
            if masked:
                scores = jnp.where(visible, scores, LOW_START)
            old_max = max_ref[:, cols]
            new_max = jnp.maximum(old_max, jnp.max(scores, axis=0, keepdims=True))
            factor = jnp.exp2((old_max - new_max) * to_exp2)
            exp_scores = jnp.exp2((scores - new_max) * to_exp2)
            max_ref[:, cols] = new_max
            sum_ref[:, cols] = sum_ref[:, cols] * factor + jnp.sum(exp_scores, axis=0, keepdims=True)
            weighted = lax.dot_general(
                value_part,
                exp_scores.astype(jnp.bfloat16),
                (((0,), (0,)), ((), ())),
                preferred_element_type=jnp.float32,
            )
            acc_ref[:, cols] = acc_ref[:, cols] * factor + weighted

    for which in range(2):
        query_block = own_ref[which]
        steps = query_block // BLOCKS_PER_STEP
        max_ref[...] = jnp.full_like(max_ref, LOW_START)
        sum_ref[...] = jnp.zeros_like(sum_ref)
        acc_ref[...] = jnp.zeros_like(acc_ref)

        @pl.loop(0, steps)
        def _(number):
            step(which, number, False, query_block)

        step(which, steps, True, query_block)
        for g in range(group):
            cols = pl.ds(g * half, half)
            attended = acc_ref[:, cols] / sum_ref[:, cols]
            out_ref[pl.ds(g * head_size, head_size), pl.ds(which * half, half)] = attended.astype(jnp.bfloat16)


def attend(query_parts, gathered, place, own, first_head, all_heads, half):
    kv_heads, _, rows, head_size = query_parts.shape
    keys_total = gathered.shape[0]
    blocks = place.shape[0]
    group = rows // half
    flops = 4 * kv_heads * rows * head_size * half * (blocks + 1)
    return pl.pallas_call(
        functools.partial(attend_kernel, half, group),
        out_shape=jax.ShapeDtypeStruct((kv_heads * group * head_size, 2 * half), jnp.bfloat16),
        grid_spec=pltpu.PrefetchScalarGridSpec(
            num_scalar_prefetch=2,
            grid=(kv_heads,),
            in_specs=[
                pl.BlockSpec((1, 2, rows, head_size), lambda h, *_: (h, 0, 0, 0)),
                pl.BlockSpec((keys_total, head_size), lambda h, *_: (0, h + first_head)),
                pl.BlockSpec((keys_total, head_size), lambda h, *_: (0, h + first_head + all_heads)),
            ],
            out_specs=pl.BlockSpec((group * head_size, 2 * half), lambda h, *_: (h, 0)),
            scratch_shapes=[
                pltpu.VMEM((head_size, rows), jnp.float32),
                pltpu.VMEM((1, rows), jnp.float32),
                pltpu.VMEM((1, rows), jnp.float32),
            ],
        ),
        compiler_params=pltpu.CompilerParams(
            dimension_semantics=("arbitrary",), vmem_limit_bytes=20 * 1024 * 1024
        ),
        cost_estimate=pl.CostEstimate(
            flops=flops, bytes_accessed=2 * gathered.size, transcendentals=flops // (4 * head_size)
        ),
        name="attend",
    )(place, own, query_parts, gathered, gathered)


def spread_kernel(devices, own_ref, out_ref, far_send, far_recv, side_send, side_recv, pair_send, pair_recv, own_sem):
    me = lax.axis_index("ctx")
    outers = devices // 4
    outer, middle, inner = me // 4, (me // 2) % 2, me % 2

    def at(o, m, i):
        return (o * 2 + m) * 2 + i

    side = at(outer, 1 - middle, inner)
    pair = at(outer, middle, 1 - inner)
    far = [at((outer + k) % outers, middle, inner) for k in range(1, outers)]
    barrier = pltpu.get_barrier_semaphore()
    for other in far + [side, pair]:
        pl.semaphore_signal(barrier, inc=1, device_id={"ctx": other}, device_id_type=pl.DeviceIdType.MESH)
    pl.semaphore_wait(barrier, outers + 1)

    def send(source, slot, sends, recvs, number, target):
        return pltpu.make_async_remote_copy(
            src_ref=source,
            dst_ref=out_ref.at[slot],
            send_sem=sends.at[number],
            recv_sem=recvs.at[number],
            device_id={"ctx": target},
            device_id_type=pl.DeviceIdType.MESH,
        )

    own = pltpu.make_async_copy(own_ref, out_ref.at[me], own_sem)
    far_copies = [send(own_ref, me, far_send, far_recv, k, far[k]) for k in range(outers - 1)]
    for copy in far_copies:
        copy.start()
    side_copies = [send(own_ref, me, side_send, side_recv, 0, side)]
    pair_copies = [send(own_ref, me, pair_send, pair_recv, 0, pair)]
    side_copies[0].start()
    pair_copies[0].start()
    own.start()
    for k in range(outers - 1):
        far_copies[k].wait_recv()
        slot = at((outer + outers - 1 - k) % outers, middle, inner)
        side_copies.append(send(out_ref.at[slot], slot, side_send, side_recv, k + 1, side))
        pair_copies.append(send(out_ref.at[slot], slot, pair_send, pair_recv, k + 1, pair))
        side_copies[-1].start()
        pair_copies[-1].start()
    for k in range(outers):
        side_copies[k].wait_recv()
        slot = at((outer + outers - k) % outers, 1 - middle, inner)
        pair_copies.append(send(out_ref.at[slot], slot, pair_send, pair_recv, outers + k, pair))
        pair_copies[-1].start()
    for copy in pair_copies:
        copy.wait_recv()
    for copy in far_copies + side_copies + pair_copies:
        copy.wait_send()
    own.wait()


def spread(packed):
    devices = lax.axis_size("ctx")
    outers = devices // 4
    rows, columns = packed.shape
    gathered = pl.pallas_call(
        functools.partial(spread_kernel, devices),
        out_shape=jax.ShapeDtypeStruct((devices, rows, columns), packed.dtype),
        in_specs=[pl.BlockSpec(memory_space=pltpu.VMEM)],
        out_specs=pl.BlockSpec(memory_space=pltpu.VMEM),
        scratch_shapes=[
            pltpu.SemaphoreType.DMA((outers - 1,)),
            pltpu.SemaphoreType.DMA((outers - 1,)),
            pltpu.SemaphoreType.DMA((outers,)),
            pltpu.SemaphoreType.DMA((outers,)),
            pltpu.SemaphoreType.DMA((2 * outers,)),
            pltpu.SemaphoreType.DMA((2 * outers,)),
            pltpu.SemaphoreType.DMA,
        ],
        compiler_params=pltpu.CompilerParams(
            collective_id=0, has_side_effects=True, vmem_limit_bytes=24 * 1024 * 1024
        ),
        cost_estimate=pl.CostEstimate(flops=0, bytes_accessed=20 * packed.size * devices, transcendentals=0),
        name="spread",
    )(packed)
    return gathered


def hand_on(value, by):
    parts = lax.axis_size("groups")
    return lax.ppermute(value, "groups", [(i, (i + by) % parts) for i in range(parts)])


def weave_kernel(share, me_ref, *refs):
    *shares, out_ref = refs
    parts = len(shares)
    for p in range(parts):
        by = lax.rem(p - me_ref[0] + parts, parts)
        chosen = shares[0][...]
        for k in range(1, parts):
            chosen = jnp.where(by == k, shares[k][...], chosen)
        for i in range(chosen.shape[1] // share):
            out_ref[:, (i * parts + p) * share : (i * parts + p + 1) * share] = chosen[:, i * share : (i + 1) * share]


def weave(results, me_part, devices):
    parts = len(results)
    tokens, columns = results[0].shape
    share = columns // devices
    return pl.pallas_call(
        functools.partial(weave_kernel, share),
        out_shape=jax.ShapeDtypeStruct((tokens, parts * columns), results[0].dtype),
        grid_spec=pltpu.PrefetchScalarGridSpec(
            num_scalar_prefetch=1,
            grid=(devices // 4,),
            in_specs=[pl.BlockSpec((tokens, 4 * share), lambda i, *_: (0, i))] * parts,
            out_specs=pl.BlockSpec((tokens, 4 * parts * share), lambda i, *_: (0, i)),
        ),
        name="weave",
    )(me_part.astype(jnp.int32).reshape(1), *results)


def local(query_states, key_states, value_rows, positions, out_weight):
    tokens, query_heads, head_size = query_states.shape
    kv_heads = key_states.shape[1]
    group = query_heads // kv_heads
    half = tokens // 2
    devices = lax.axis_size("ctx")
    blocks = 2 * devices
    parts = lax.axis_size("groups")
    me_part = lax.axis_index("groups")
    share = out_weight.shape[1] // parts
    weight_share = lax.dynamic_slice_in_dim(out_weight, me_part * share, share, 1)
    weight = lax.all_gather(weight_share, "ctx", axis=1, tiled=True)
    packed = jnp.concatenate(
        [key_states.reshape(tokens, kv_heads * head_size), value_rows.reshape(tokens, kv_heads * head_size)], axis=1
    )
    first = positions[0] // half
    tail = jnp.broadcast_to(first.astype(packed.dtype), (TAIL, packed.shape[1]))
    gathered = spread(jnp.concatenate([packed, tail], axis=0))
    firsts = gathered[:, tokens, 0].astype(jnp.int32)
    gathered = gathered.reshape(devices * (tokens + TAIL), packed.shape[1])
    wanted = jnp.arange(blocks, dtype=jnp.int32)[:, None]
    stored = jnp.stack([firsts, blocks - 1 - firsts], axis=1).reshape(1, blocks)
    kept = jnp.arange(blocks, dtype=jnp.int32)[None, :]
    starts = kept // 2 * (tokens + TAIL) + kept % 2 * half
    place = jnp.sum(jnp.where(stored == wanted, starts, 0), axis=1)
    place = place.astype(jnp.int32)
    own = jnp.stack([first, blocks - 1 - first]).astype(jnp.int32)
    query_parts = query_states.reshape(2, half, kv_heads, group, head_size).transpose(2, 0, 3, 1, 4)
    query_parts = query_parts.reshape(kv_heads, 2, group * half, head_size)
    pieces = min(2, kv_heads)
    span = kv_heads // pieces
    attended = [
        attend(query_parts[i * span : (i + 1) * span], gathered, place, own, i * span, kv_heads, half) for i in range(pieces)
    ]

    def project(rows):
        product = lax.dot_general(
            jnp.concatenate(rows, axis=0), weight, (((0,), (0,)), ((), ())), preferred_element_type=jnp.float32
        )
        return product.astype(jnp.bfloat16)

    guests = [[hand_on(piece, by) for piece in attended] for by in range(1, parts)]
    mine = project(attended)
    results = [mine] + [hand_on(project(rows), parts - 1 - i) for i, rows in enumerate(guests)]
    if share % 128 == 0:
        combined = weave(results, me_part, devices)
    else:
        shares = jnp.stack([r.reshape(tokens, devices, share) for r in results])
        order = (jnp.arange(parts) - me_part) % parts
        combined = jnp.moveaxis(jnp.take(shares, order, axis=0), 0, 2).reshape(tokens, devices * parts * share)
    return lax.psum_scatter(combined, "tp", scatter_dimension=1, tiled=True)


def solution(mesh):
    in_specs = (
        P(("groups", "ctx"), "tp", None),
        P(("groups", "ctx"), "tp", None),
        P(("groups", "ctx"), "tp", None),
        P(("groups", "ctx")),
        P("tp", "ctx"),
    )
    out_specs = P(("groups", "ctx"), "tp")
    return jax.shard_map(local, mesh=mesh, in_specs=in_specs, out_specs=out_specs, check_vma=False)
```
